32 devices in a mesh: frame: 16 (over z, y, core), clip: 2 (over x).
Axes of the slice: x: 2, y: 2, z: 4, core: 2. Of those that a mesh axis runs over, the one named last changes fastest.
Arguments:
- patches: bfloat16 [4, 16, 144, 1152], P('clip', 'frame'), may hold values from -4 to 4
- captions: bfloat16 [4, 120, 1152], P('clip'), may hold values from -4 to 4
- caption_lengths: int32 [4], P('clip'), may hold values from 5 to 120, as said below
- timestep_signal: float32 [4, 6912], P('clip'), may hold values from -1 to 1
- spatial_input: bfloat16 [1152, 3456], P('frame', 'clip'), may hold values from -0.1875 to 0.1875
- spatial_output: bfloat16 [1152, 1152], P('frame', 'clip'), may hold values from -0.625 to 0.625
- temporal_input: bfloat16 [1152, 3456], P('frame', 'clip'), may hold values from -0.1875 to 0.1875
- temporal_output: bfloat16 [1152, 1152], P('frame', 'clip'), may hold values from -0.4375 to 0.4375
- cross_query: bfloat16 [1152, 1152], P('frame', 'clip'), may hold values from -0.1875 to 0.1875
- cross_keyvalue: bfloat16 [1152, 2304], P('frame', 'clip'), may hold values from -0.1875 to 0.1875
- cross_output: bfloat16 [1152, 1152], P('frame', 'clip'), may hold values from -0.5 to 0.5
- expand_weight: bfloat16 [1152, 4608], P('frame', 'clip'), may hold values from -0.1875 to 0.1875
- contract_weight: bfloat16 [4608, 1152], P('frame', 'clip'), may hold values from -0.09375 to 0.09375
- bias_vector: bfloat16 [16128], P(('frame', 'clip')), may hold values from -1 to 1
- modulation_table: bfloat16 [6912], P(('frame', 'clip')), may hold values from -0.59765625 to 0.59765625
- cotangent: bfloat16 [4, 16, 144, 1152], P('clip', 'frame'), may hold values from -6 to 6
Outputs:
- output: bfloat16 [4, 16, 144, 1152], P('clip', 'frame')
- patch_gradient: float32 [4, 16, 144, 1152], P('clip', 'frame')
- caption_gradient: float32 [4, 120, 1152], P('clip')
- timestep_gradient: float32 [4, 6912], P('clip')
- spatial_input_gradient: float32 [1152, 3456], P('frame', 'clip')
- spatial_output_gradient: float32 [1152, 1152], P('frame', 'clip')
- temporal_input_gradient: float32 [1152, 3456], P('frame', 'clip')
- temporal_output_gradient: float32 [1152, 1152], P('frame', 'clip')
- cross_query_gradient: float32 [1152, 1152], P('frame', 'clip')
- cross_keyvalue_gradient: float32 [1152, 2304], P('frame', 'clip')
- cross_output_gradient: float32 [1152, 1152], P('frame', 'clip')
- expand_gradient: float32 [1152, 4608], P('frame', 'clip')
- contract_gradient: float32 [4608, 1152], P('frame', 'clip')
- bias_gradient: float32 [16128], P(('frame', 'clip'))
- table_gradient: float32 [6912], P(('frame', 'clip'))
The draws below stay inside these ranges and needn't reach their ends.
Inputs may be any that keep to these rules, and one draw needn't show every extreme that they name: `caption_lengths`: caption slots in use per clip; in every draw some clip uses all 120 slots and another uses 5.
All inputs are finite; a program needn't handle non-finite values.
Results may differ from the reference program's by a relative error of at most 0.03.
Values may be sent and summed in bfloat16 or wider, within the bound.
A program may use at most 256 MiB of HBM per device.

```python
import jax
import jax.numpy as jnp
from jax import lax

D = 1152
HEADS = 16
HEAD_DIM = 72
FF = 4608
LTXT = 120
S = 144
FRAMES = 16
CLIPS = 4
NBIAS = 16128
NMOD = 6912


def draw_caption_lengths(key, part):
    first_key, second_key, third_key = jax.random.split(jax.random.fold_in(key, 17), 3)
    drawn = jax.random.randint(first_key, (CLIPS,), 5, LTXT + 1)
    longest = jax.random.randint(second_key, (), 0, CLIPS)
    offset = jax.random.randint(third_key, (), 1, CLIPS)
    shortest = (longest + offset) % CLIPS
    position = jnp.arange(CLIPS)
    return jnp.where(position == longest, LTXT, jnp.where(position == shortest, 5, drawn)).astype(jnp.int32)


def unit_field(key, shape):
    values = jnp.clip(jax.random.normal(key, shape, jnp.float32), -4.0, 4.0)
    return values


def draw_patches(key, part):
    return unit_field(jax.random.fold_in(key, 31), (CLIPS, FRAMES, S, D)).astype(jnp.bfloat16)


def draw_captions(key, part):
    return unit_field(jax.random.fold_in(key, 37), (CLIPS, LTXT, D)).astype(jnp.bfloat16)


def draw_timestep_signal(key, part):
    inner = jax.random.fold_in(key, 41)
    values = jnp.clip(0.4 * jax.random.normal(inner, (CLIPS, NMOD), jnp.float32), -1.0, 1.0)
    return values


def levels(own_key, extent, cuts, least, top_value):
    gain = 1.0
    for dim, blocks in cuts:
        steps = jax.random.uniform(jax.random.fold_in(jax.random.fold_in(own_key, 6), dim), (blocks,), jnp.float32, least / len(cuts), top_value / len(cuts))
        gain = gain * jnp.repeat(jnp.exp(steps), extent[dim] // blocks).reshape((-1,) + (1,) * (len(extent) - 1 - dim))
    return gain


def gaussian(stream_key, dims, deviation, most, cuts=(), held_as=jnp.bfloat16):
    array = jax.random.normal(stream_key, dims, jnp.float32) * deviation
    if len(cuts) > 0:
        array = levels(stream_key, dims, cuts, -0.22, 0.18) * array
    return jnp.clip(array, min=-most, max=most).astype(held_as)


def setup_inputs(seed: int = 0) -> dict:
    keys = jax.random.split(jax.random.key(seed), 17)
    patches = draw_patches(jax.random.fold_in(keys[16], 71), 0)
    captions = draw_captions(jax.random.fold_in(keys[16], 71), 0)
    caption_lengths = draw_caption_lengths(jax.random.fold_in(keys[16], 71), 0)
    timestep_signal = draw_timestep_signal(jax.random.fold_in(keys[16], 71), 0)
    spatial_input = gaussian(keys[4], (D, 3 * D), D ** -0.5, 0.1875, ((0, 16), (1, 2)))
    spatial_output = gaussian(keys[5], (D, D), (D // 12) ** -0.5, 0.625, ((0, 16), (1, 2)))
    temporal_input = gaussian(keys[6], (D, 3 * D), D ** -0.5, 0.1875, ((0, 16), (1, 2)))
    temporal_output = gaussian(keys[7], (D, D), (D // 6) ** -0.5, 0.4375, ((0, 16), (1, 2)))
    cross_query = gaussian(keys[8], (D, D), D ** -0.5, 0.1875, ((0, 16), (1, 2)))
    cross_keyvalue = gaussian(keys[9], (D, 2 * D), D ** -0.5, 0.1875, ((0, 16), (1, 2)))
    cross_output = gaussian(keys[10], (D, D), (D // 8) ** -0.5, 0.5, ((0, 16), (1, 2)))
    expand_weight = gaussian(keys[11], (D, FF), D ** -0.5, 0.1875, ((0, 16), (1, 2)))
    contract_weight = gaussian(keys[12], (FF, D), FF ** -0.5, 0.09375, ((0, 16), (1, 2)))
    bias_vector = gaussian(keys[13], (NBIAS,), 0.3, 1.0, ((0, 32),))
    modulation_table = gaussian(keys[14], (NMOD,), 0.2, 0.59765625, ((0, 32),))
    cotangent = gaussian(keys[15], (CLIPS, FRAMES, S, D), 1.0, 6.0, ((0, 2), (1, 16)))
    return dict(patches=patches, captions=captions, caption_lengths=caption_lengths, timestep_signal=timestep_signal, spatial_input=spatial_input, spatial_output=spatial_output, temporal_input=temporal_input, temporal_output=temporal_output, cross_query=cross_query, cross_keyvalue=cross_keyvalue, cross_output=cross_output, expand_weight=expand_weight, contract_weight=contract_weight, bias_vector=bias_vector, modulation_table=modulation_table, cotangent=cotangent)


@jax.custom_vjp
def low(v):
    return lax.optimization_barrier(v.astype(jnp.bfloat16)).astype(jnp.float32)

@jax.custom_vjp
def low_back(v):
    return v

def low_keep(v):
    return (low(v), None)

def low_pass(kept, grad):
    return (grad,)

def back_keep(v):
    return (v, None)

def back_low(kept, grad):
    return (low(grad),)
low.defvjp(low_keep, low_pass)
low_back.defvjp(back_keep, back_low)
norm_eps = 1e-06
masked_score = -1000000000.0

def layer_norm(values):
    centred = values - lax.optimization_barrier(jnp.mean(values, axis=-1, keepdims=True))
    return centred * lax.rsqrt(lax.optimization_barrier(jnp.mean(centred * centred, axis=-1, keepdims=True)) + norm_eps)

def matmul(left, right):
    return jnp.dot(left, right, precision=lax.Precision.HIGHEST)

def attend(queries, key_rows, value_rows, valid):
    scores = jnp.einsum('bqhd,bkhd->bhqk', queries, key_rows, precision=lax.Precision.HIGHEST) * HEAD_DIM ** (-0.5)
    if valid is not None:
        scores = jnp.where(valid, scores, masked_score)
    probabilities = low(jax.nn.softmax(low_back(scores), axis=-1))
    result = jnp.einsum('bhqk,bkhd->bqhd', probabilities, value_rows, precision=lax.Precision.HIGHEST)
    return low(low_back(result))

def clip_forward(patch_rows, caption_rows, time_row, length, matrices, bias_all, mod_table):
    spatial_in_w, spatial_out_w, temporal_in_w, temporal_out_w, cross_query_w, cross_pair_w, cross_out_w, expand_w, contract_w = matrices
    frames = patch_rows.shape[0]
    modulation = mod_table.reshape(6, D) + time_row.reshape(6, D)
    zero_block = jnp.zeros((D,), jnp.float32)
    spatial_bias = jnp.concatenate([bias_all[0:D], zero_block, bias_all[D:2 * D]])
    temporal_bias = jnp.concatenate([bias_all[3 * D:4 * D], zero_block, bias_all[4 * D:5 * D]])
    pair_bias = jnp.concatenate([zero_block, bias_all[7 * D:8 * D]])
    spatial_in = low(layer_norm(patch_rows) * (1.0 + modulation[1]) + modulation[0])
    spatial_pack = low(low_back(matmul(spatial_in, spatial_in_w) + spatial_bias)).reshape(frames, S, 3, HEADS, HEAD_DIM)
    spatial_att = attend(spatial_pack[:, :, 0], spatial_pack[:, :, 1], spatial_pack[:, :, 2], None).reshape(frames, S, D)
    spatial_out = low_back(matmul(spatial_att, spatial_out_w) + bias_all[2 * D:3 * D])
    after_spatial = patch_rows + modulation[2] * spatial_out
    temporal_in = low_back(low(jnp.transpose(after_spatial, (1, 0, 2))))
    temporal_pack = low(low_back(matmul(temporal_in, temporal_in_w) + temporal_bias)).reshape(S, frames, 3, HEADS, HEAD_DIM)
    temporal_att = attend(temporal_pack[:, :, 0], temporal_pack[:, :, 1], temporal_pack[:, :, 2], None).reshape(S, frames, D)
    temporal_out = low(low_back(matmul(temporal_att, temporal_out_w) + bias_all[5 * D:6 * D]))
    after_temporal = after_spatial + modulation[2] * jnp.transpose(temporal_out, (1, 0, 2))
    cross_in = low(after_temporal)
    cross_queries = low(low_back(matmul(cross_in, cross_query_w) + bias_all[6 * D:7 * D])).reshape(1, frames * S, HEADS, HEAD_DIM)
    cross_pairs = low(low_back(matmul(caption_rows, cross_pair_w) + pair_bias)).reshape(1, LTXT, 2, HEADS, HEAD_DIM)
    valid = (jnp.arange(LTXT) < length)[None, None, None, :]
    cross_att = attend(cross_queries, cross_pairs[:, :, 0], cross_pairs[:, :, 1], valid).reshape(frames, S, D)
    cross_out = low_back(matmul(cross_att, cross_out_w) + bias_all[8 * D:9 * D])
    after_cross = after_temporal + cross_out
    mlp_in = low(layer_norm(after_cross) * (1.0 + modulation[4]) + modulation[3])
    hidden_pre = low_back(matmul(mlp_in, expand_w) + bias_all[9 * D:9 * D + FF])
    hidden_act = low(jax.nn.gelu(hidden_pre, approximate=True))
    mixed = low_back(matmul(hidden_act, contract_w) + bias_all[9 * D + FF:10 * D + FF])
    return after_cross + modulation[5] * mixed

def add_pair(first, second):
    return first + second

def reference(patches, captions, caption_lengths, timestep_signal, spatial_input, spatial_output, temporal_input, temporal_output, cross_query, cross_keyvalue, cross_output, expand_weight, contract_weight, bias_vector, modulation_table, cotangent):
    matrices = tuple((matrix.astype(jnp.float32) for matrix in (spatial_input, spatial_output, temporal_input, temporal_output, cross_query, cross_keyvalue, cross_output, expand_weight, contract_weight)))
    bias_all = bias_vector.astype(jnp.float32)
    mod_table = modulation_table.astype(jnp.float32)

    def one_clip(totals, inputs):
        patch_rows, caption_rows, time_row, length, upstream = inputs

        def forward(patch_rows, caption_rows, time_row, matrices, bias_all, mod_table):
            return clip_forward(patch_rows, caption_rows, time_row, length, matrices, bias_all, mod_table)
        result, backward = jax.vjp(forward, patch_rows, caption_rows, time_row, matrices, bias_all, mod_table)
        gradients = backward(upstream)
        totals = jax.tree.map(add_pair, totals, (gradients[3], gradients[4], gradients[5]))
        return (totals, (result.astype(jnp.bfloat16), gradients[0], gradients[1], gradients[2]))
    initial = jax.tree.map(jnp.zeros_like, (matrices, bias_all, mod_table))
    totals, stacked = lax.scan(one_clip, initial, (patches.astype(jnp.float32), captions.astype(jnp.float32), timestep_signal, caption_lengths, cotangent.astype(jnp.float32)))
    weights_grads = totals[0]
    return (stacked[0], stacked[1], stacked[2], stacked[3], weights_grads[0], weights_grads[1], weights_grads[2], weights_grads[3], weights_grads[4], weights_grads[5], weights_grads[6], weights_grads[7], weights_grads[8], totals[1], totals[2])
```

```python
from functools import partial

import jax
import jax.numpy as jnp
from jax import lax
from jax.sharding import PartitionSpec as P


D = 1152
HEADS = 16
HEAD_DIM = 72
FF = 4608


norm_eps = 1e-06
masked_score = -1000000000.0


def normalize(values):
    centred = values - jnp.mean(values, axis=-1, keepdims=True)
    inverse = lax.rsqrt(jnp.mean(centred * centred, axis=-1, keepdims=True) + norm_eps)
    return (centred * inverse, inverse)


def normalize_back(normed, inverse, upstream):
    return inverse * (
        upstream
        - jnp.mean(upstream, axis=-1, keepdims=True)
        - normed * jnp.mean(upstream * normed, axis=-1, keepdims=True)
    )


def score_block(queries, key_rows, valid):
    scores = jnp.einsum(
        "bqhd,bkhd->bhqk", queries, key_rows, preferred_element_type=jnp.float32
    ) * HEAD_DIM ** (-0.5)
    if valid is None:
        return scores
    return jnp.where(valid, scores, masked_score)


def attend_forward(queries, key_rows, value_rows, valid):
    scores = score_block(queries, key_rows, valid)
    highest = jnp.max(scores, axis=-1, keepdims=True)
    exponent = jnp.exp(scores - highest)
    denominator = jnp.sum(exponent, axis=-1, keepdims=True)
    probabilities = (exponent / denominator).astype(jnp.bfloat16)
    result = jnp.einsum(
        "bhqk,bkhd->bqhd", probabilities, value_rows, preferred_element_type=jnp.float32
    )
    return (result.astype(jnp.bfloat16), highest + jnp.log(denominator))


def attend_backward(queries, key_rows, value_rows, valid, log_total, result_grad):
    probabilities = jnp.exp(score_block(queries, key_rows, valid) - log_total)
    prob_grad = jnp.einsum(
        "bqhd,bkhd->bhqk", result_grad, value_rows, preferred_element_type=jnp.float32
    )
    value_grad = jnp.einsum(
        "bhqk,bqhd->bkhd",
        probabilities.astype(jnp.bfloat16),
        result_grad,
        preferred_element_type=jnp.float32,
    )
    score_grad = probabilities * (
        prob_grad - jnp.sum(probabilities * prob_grad, axis=-1, keepdims=True)
    )
    score_grad = score_grad.astype(jnp.bfloat16)
    query_grad = jnp.einsum(
        "bhqk,bkhd->bqhd", score_grad, key_rows, preferred_element_type=jnp.float32
    ) * HEAD_DIM ** (-0.5)
    key_grad = jnp.einsum(
        "bhqk,bqhd->bkhd", score_grad, queries, preferred_element_type=jnp.float32
    ) * HEAD_DIM ** (-0.5)
    return (query_grad, key_grad, value_grad)


def project(inputs, matrix, offset):
    return jnp.dot(inputs, matrix, preferred_element_type=jnp.float32) + offset


def gather_matrix(matrix):
    blocks = lax.all_gather(matrix, ("frame", "clip"), axis=0)
    rows, columns = matrix.shape
    frames, clips = (lax.axis_size("frame"), lax.axis_size("clip"))
    blocks = blocks.reshape(frames, clips, rows, columns)
    return jnp.transpose(blocks, (0, 2, 1, 3)).reshape(frames * rows, clips * columns)


def padded_row(values, total):
    return jnp.pad(values, ((0, 0), (0, total - values.shape[1])))


def gather_vectors(first, second):
    one, two = (first.shape[0], second.shape[0])
    total = -(-(one + two) // 1024) * 1024
    row = padded_row(jnp.concatenate([first, second])[None], total).reshape(total // 128, 128)
    blocks = lax.all_gather(row, ("frame", "clip"), axis=0).reshape(-1, total)
    return blocks[:, :one].reshape(-1), blocks[:, one : one + two].reshape(-1)


def bit_count(size):
    return size.bit_length() - 1


def mine(axis, bit):
    return lax.rem(lax.shift_right_logical(lax.axis_index(axis), bit), 2)


def swap(values, axis, bit):
    size = lax.axis_size(axis)
    return lax.ppermute(values, axis, [(i, i ^ (1 << bit)) for i in range(size)])


def dims_of(axes):
    return [(axis, bit) for axis in axes for bit in reversed(range(bit_count(lax.axis_size(axis))))]


def pick(values, dims, entry, index):
    at = dims.index(entry)
    return lax.dynamic_index_in_dim(values, index, at, keepdims=False), dims[:at] + dims[at + 1 :]


def halve(values, dims, entry):
    axis, bit = entry
    own = mine(axis, bit)
    away, _ = pick(values, dims, entry, 1 - own)
    keep, rest = pick(values, dims, entry, own)
    return (keep + swap(away, axis, bit)).astype(values.dtype), rest


def scatter_sum(values, dims, order):
    for entry in order:
        values, dims = halve(values, dims, entry)
    return values


def full_order(lead):
    every = dims_of(("clip", "frame"))[::-1]
    frame_bits = sorted((e for e in every if e[0] == "frame"), key=lambda e: e[1])
    clip_bits = [e for e in every if e[0] == "clip"]
    core, y_bit, z_bits = frame_bits[:1], frame_bits[1:2], frame_bits[2:]
    if lead == "clip":
        return core + clip_bits + y_bit + z_bits
    if lead == "y":
        return core + y_bit + clip_bits + z_bits
    return core + z_bits + clip_bits + y_bit


def weight_grad(inputs, upstream, lead="clip"):
    frames, clips = (lax.axis_size("frame"), lax.axis_size("clip"))
    tokens = inputs.shape[0]
    rows, columns = (inputs.shape[1] // frames, upstream.shape[1] // clips)
    left = inputs.T.reshape((2,) * bit_count(frames) + (rows, tokens))
    right = jnp.transpose(upstream.reshape(tokens, clips, columns), (1, 0, 2)).reshape(
        (2,) * bit_count(clips) + (tokens, columns)
    )
    frame_dims, clip_dims = (dims_of(("frame",)), dims_of(("clip",)))
    order = full_order(lead)
    first, second = order[:2]

    def block(chosen):
        l_val, l_dims, r_val, r_dims = left, frame_dims, right, clip_dims
        for entry, index in chosen:
            if entry[0] == "frame":
                l_val, l_dims = pick(l_val, l_dims, entry, index)
            else:
                r_val, r_dims = pick(r_val, r_dims, entry, index)
        flat_left = l_val.reshape(-1, tokens)
        flat_right = r_val.reshape(-1, tokens, columns)
        parts = [
            jnp.dot(flat_left, flat_right[i], preferred_element_type=jnp.float32)
            for i in range(flat_right.shape[0])
        ]
        return parts, l_dims, r_dims

    def shaped(parts, l_dims, r_dims):
        value = parts[0][None] if len(parts) == 1 else jnp.stack(parts)
        return value.reshape((2,) * (len(r_dims) + len(l_dims)) + (rows, columns))

    own_first, own_second = (mine(*first), mine(*second))
    other = block([(first, 1 - own_first), (second, 1 - own_second)])
    other_kept = block([(first, 1 - own_first), (second, own_second)])
    here = block([(first, own_first), (second, 1 - own_second)])
    kept = block([(first, own_first), (second, own_second)])
    came = swap(shaped(*other).astype(jnp.bfloat16), *first)
    came_kept = swap(shaped(*other_kept).astype(jnp.bfloat16), *first)
    away = (shaped(*here) + came.astype(jnp.float32)).astype(jnp.bfloat16)
    value = shaped(*kept) + came_kept.astype(jnp.float32)
    value = (value + swap(away, *second).astype(jnp.float32)).astype(jnp.bfloat16)
    dims = kept[2] + kept[1]
    return scatter_sum(value, dims, order[2:]).astype(jnp.float32)


def reduce_columns(values):
    clips = lax.axis_size("clip")
    rows, columns = (values.shape[0], values.shape[1] // clips)
    blocks = jnp.transpose(values.astype(jnp.bfloat16).reshape(rows, clips, columns), (1, 0, 2))
    dims = dims_of(("clip",))
    blocks = blocks.reshape((2,) * len(dims) + (rows, columns))
    return scatter_sum(blocks, dims, dims).astype(jnp.float32)


def reduce_vectors(first, second):
    devices = lax.axis_size("frame") * lax.axis_size("clip")
    one, two = (first.shape[0] // devices, second.shape[0] // devices)
    total = -(-(one + two) // 1024) * 1024
    both = jnp.concatenate([first.reshape(devices, one), second.reshape(devices, two)], axis=1)
    dims = dims_of(("frame", "clip"))
    blocks = padded_row(both, total).reshape((2,) * len(dims) + (total // 128, 128))
    row = scatter_sum(blocks, dims, full_order("clip")).reshape(-1)
    return row[:one], row[one : one + two]


def frame_total(values):
    frames = lax.axis_size("frame")
    rows = values.shape[0]
    each = -(-rows // frames)
    each = -(-each // 8) * 8
    blocks = jnp.pad(values, ((0, each * frames - rows), (0, 0)))
    own = lax.psum_scatter(blocks, "frame", scatter_dimension=0, tiled=True)
    return lax.all_gather(own, "frame", axis=0, tiled=True)[:rows]


def input_grad(upstream, matrix):
    return jnp.einsum("ro,io->ri", upstream, matrix, preferred_element_type=jnp.float32)


def column_sum(upstream):
    return jnp.sum(upstream.astype(jnp.float32), axis=0)


def clip_sum(values):
    return jnp.sum(values, axis=(1, 2))


def per_device(
    patches,
    captions,
    caption_lengths,
    timestep_signal,
    spatial_input,
    spatial_output,
    temporal_input,
    temporal_output,
    cross_query,
    cross_keyvalue,
    cross_output,
    expand_weight,
    contract_weight,
    bias_vector,
    modulation_table,
    cotangent,
):
    gathered = tuple(
        gather_matrix(matrix)
        for matrix in (
            spatial_input,
            spatial_output,
            temporal_input,
            temporal_output,
            cross_query,
            cross_keyvalue,
            cross_output,
            expand_weight,
            contract_weight,
        )
    )
    bias_full, table_full = gather_vectors(bias_vector, modulation_table)
    bias_full = bias_full.astype(jnp.float32)
    clip_local, frame_local, patch_local = (patches.shape[0], patches.shape[1], patches.shape[2])
    frame_size = lax.axis_size("frame")
    modulation = table_full.astype(jnp.float32).reshape(1, 6, D) + timestep_signal.reshape(
        clip_local, 6, D
    )
    shift_first = modulation[:, 0][:, None, None, :]
    scale_first = modulation[:, 1][:, None, None, :]
    gate_first = modulation[:, 2][:, None, None, :]
    shift_second = modulation[:, 3][:, None, None, :]
    scale_second = modulation[:, 4][:, None, None, :]
    gate_second = modulation[:, 5][:, None, None, :]
    zero_block = jnp.zeros((D,), jnp.float32)
    spatial_bias = jnp.concatenate([bias_full[0:D], zero_block, bias_full[D : 2 * D]])
    temporal_bias = jnp.concatenate(
        [bias_full[3 * D : 4 * D], zero_block, bias_full[4 * D : 5 * D]]
    )
    pair_bias = jnp.concatenate([zero_block, bias_full[7 * D : 8 * D]])
    values = patches.astype(jnp.float32)
    normed_first, inverse_first = normalize(values)
    spatial_in = (
        (normed_first * (1.0 + scale_first) + shift_first).astype(jnp.bfloat16).reshape(-1, D)
    )
    spatial_pack = (
        project(spatial_in, gathered[0], spatial_bias)
        .astype(jnp.bfloat16)
        .reshape(clip_local * frame_local, patch_local, 3, HEADS, HEAD_DIM)
    )
    spatial_att, spatial_total = attend_forward(
        spatial_pack[:, :, 0], spatial_pack[:, :, 1], spatial_pack[:, :, 2], None
    )
    spatial_att = spatial_att.reshape(-1, D)
    spatial_out = project(spatial_att, gathered[1], bias_full[2 * D : 3 * D]).reshape(values.shape)
    after_spatial = values + gate_first * spatial_out
    outgoing = jnp.transpose(after_spatial.astype(jnp.bfloat16), (0, 2, 1, 3)).reshape(
        clip_local * patch_local, frame_local, D
    )
    by_position = lax.all_to_all(outgoing, "frame", split_axis=0, concat_axis=1, tiled=True)
    position_count, frame_count = (by_position.shape[0], by_position.shape[1])
    position_rows = by_position.reshape(-1, D)
    temporal_pack = (
        project(position_rows, gathered[2], temporal_bias)
        .astype(jnp.bfloat16)
        .reshape(position_count, frame_count, 3, HEADS, HEAD_DIM)
    )
    temporal_att, temporal_total = attend_forward(
        temporal_pack[:, :, 0], temporal_pack[:, :, 1], temporal_pack[:, :, 2], None
    )
    temporal_att = temporal_att.reshape(-1, D)
    temporal_out = (
        project(temporal_att, gathered[3], bias_full[5 * D : 6 * D])
        .astype(jnp.bfloat16)
        .reshape(position_count, frame_count, D)
    )
    returned = lax.all_to_all(temporal_out, "frame", split_axis=1, concat_axis=0, tiled=True)
    temporal_back = jnp.transpose(
        returned.reshape(clip_local, patch_local, frame_local, D), (0, 2, 1, 3)
    ).astype(jnp.float32)
    after_temporal = after_spatial + gate_first * temporal_back
    cross_in = after_temporal.astype(jnp.bfloat16).reshape(-1, D)
    cross_queries = (
        project(cross_in, gathered[4], bias_full[6 * D : 7 * D])
        .astype(jnp.bfloat16)
        .reshape(clip_local, frame_local * patch_local, HEADS, HEAD_DIM)
    )
    text_slots = captions.shape[1]
    cross_pairs = (
        project(captions.reshape(-1, D), gathered[5], pair_bias)
        .astype(jnp.bfloat16)
        .reshape(clip_local, text_slots, 2, HEADS, HEAD_DIM)
    )
    valid = (jnp.arange(text_slots, dtype=jnp.int32)[None, :] < caption_lengths[:, None])[
        :, None, None, :
    ]
    cross_att, cross_total = attend_forward(
        cross_queries, cross_pairs[:, :, 0], cross_pairs[:, :, 1], valid
    )
    cross_att = cross_att.reshape(-1, D)
    cross_out = project(cross_att, gathered[6], bias_full[8 * D : 9 * D]).reshape(values.shape)
    after_cross = after_temporal + cross_out
    normed_second, inverse_second = normalize(after_cross)
    mlp_in = (
        (normed_second * (1.0 + scale_second) + shift_second).astype(jnp.bfloat16).reshape(-1, D)
    )
    hidden_pre = project(mlp_in, gathered[7], bias_full[9 * D : 9 * D + FF])
    hidden_act = jax.nn.gelu(hidden_pre, approximate=True).astype(jnp.bfloat16)
    mixed = project(hidden_act, gathered[8], bias_full[9 * D + FF : 10 * D + FF]).reshape(
        values.shape
    )
    output = (after_cross + gate_second * mixed).astype(jnp.bfloat16)
    matrices = gathered
    upstream = cotangent.astype(jnp.float32)
    mixed_grad = (gate_second * upstream).astype(jnp.bfloat16).reshape(-1, D)
    gate_second_grad = clip_sum(upstream * mixed)
    contract_grad = weight_grad(hidden_act, mixed_grad, "z")
    contract_bias = column_sum(mixed_grad)
    gelu_back = jax.vjp(partial(jax.nn.gelu, approximate=True), hidden_pre)[1]
    hidden_grad = gelu_back(input_grad(mixed_grad, matrices[8]))[0].astype(jnp.bfloat16)
    expand_grad = weight_grad(mlp_in, hidden_grad, "clip")
    expand_bias = column_sum(hidden_grad)
    mlp_in_grad = input_grad(hidden_grad, matrices[7]).reshape(values.shape)
    scale_second_grad = clip_sum(mlp_in_grad * normed_second)
    shift_second_grad = clip_sum(mlp_in_grad)
    cross_grad_full = upstream + normalize_back(
        normed_second, inverse_second, mlp_in_grad * (1.0 + scale_second)
    )
    cross_out_grad = cross_grad_full.astype(jnp.bfloat16).reshape(-1, D)
    cross_output_grad = weight_grad(cross_att, cross_out_grad, "y")
    cross_output_bias = column_sum(cross_out_grad)
    cross_att_grad = (
        input_grad(cross_out_grad, matrices[6])
        .astype(jnp.bfloat16)
        .reshape(clip_local, frame_local * patch_local, HEADS, HEAD_DIM)
    )
    query_part, key_part, value_part = attend_backward(
        cross_queries,
        cross_pairs[:, :, 0],
        cross_pairs[:, :, 1],
        valid,
        cross_total,
        cross_att_grad,
    )
    query_part = query_part.astype(jnp.bfloat16).reshape(-1, D)
    cross_query_grad = weight_grad(cross_in, query_part, "y")
    cross_query_bias = column_sum(query_part)
    temporal_grad_full = cross_grad_full + input_grad(query_part, matrices[4]).reshape(values.shape)
    pair_partial = jnp.stack([key_part, value_part], axis=2).reshape(clip_local, text_slots, 2 * D)
    pair_total = frame_total(pair_partial.reshape(-1, 2 * D).astype(jnp.bfloat16)).reshape(
        pair_partial.shape
    )
    caption_gradient = jnp.einsum(
        "clo,io->cli", pair_total, matrices[5], preferred_element_type=jnp.float32
    )
    row_width = D // frame_size
    caption_rows = lax.dynamic_slice_in_dim(
        captions, lax.axis_index("frame") * row_width, row_width, 2
    )
    pair_weight_grad = jnp.einsum(
        "cli,clo->io", caption_rows, pair_total, preferred_element_type=jnp.float32
    )
    pair_value_bias = jnp.sum(pair_total[:, :, D:].astype(jnp.float32), axis=(0, 1))
    pair_value_bias = jnp.where(
        lax.axis_index("frame") == 0, pair_value_bias, jnp.zeros_like(pair_value_bias)
    )
    temporal_out_grad = (gate_first * temporal_grad_full).astype(jnp.bfloat16)
    gate_first_grad = clip_sum(temporal_grad_full * temporal_back)
    outgoing_grad = jnp.transpose(temporal_out_grad, (0, 2, 1, 3)).reshape(
        clip_local * patch_local, frame_local, D
    )
    position_grad = lax.all_to_all(
        outgoing_grad, "frame", split_axis=0, concat_axis=1, tiled=True
    ).reshape(-1, D)
    temporal_output_grad = weight_grad(temporal_att, position_grad, "y")
    temporal_output_bias = column_sum(position_grad)
    temporal_att_grad = (
        input_grad(position_grad, matrices[3])
        .astype(jnp.bfloat16)
        .reshape(position_count, frame_count, HEADS, HEAD_DIM)
    )
    temporal_parts = attend_backward(
        temporal_pack[:, :, 0],
        temporal_pack[:, :, 1],
        temporal_pack[:, :, 2],
        None,
        temporal_total,
        temporal_att_grad,
    )
    temporal_pack_grad = jnp.stack(temporal_parts, axis=2).astype(jnp.bfloat16).reshape(-1, 3 * D)
    temporal_input_grad = weight_grad(position_rows, temporal_pack_grad, "y")
    temporal_query_bias = column_sum(temporal_pack_grad[:, 0:D])
    temporal_value_bias = column_sum(temporal_pack_grad[:, 2 * D : 3 * D])
    position_in_grad = (
        input_grad(temporal_pack_grad, matrices[2])
        .astype(jnp.bfloat16)
        .reshape(position_count, frame_count, D)
    )
    returned_grad = lax.all_to_all(
        position_in_grad, "frame", split_axis=1, concat_axis=0, tiled=True
    )
    spatial_grad_full = temporal_grad_full + jnp.transpose(
        returned_grad.reshape(clip_local, patch_local, frame_local, D), (0, 2, 1, 3)
    ).astype(jnp.float32)
    spatial_out_grad = (gate_first * spatial_grad_full).astype(jnp.bfloat16).reshape(-1, D)
    gate_first_grad = gate_first_grad + clip_sum(spatial_grad_full * spatial_out)
    spatial_output_grad = weight_grad(spatial_att, spatial_out_grad, "y")
    spatial_output_bias = column_sum(spatial_out_grad)
    spatial_att_grad = (
        input_grad(spatial_out_grad, matrices[1])
        .astype(jnp.bfloat16)
        .reshape(clip_local * frame_local, patch_local, HEADS, HEAD_DIM)
    )
    spatial_parts = attend_backward(
        spatial_pack[:, :, 0],
        spatial_pack[:, :, 1],
        spatial_pack[:, :, 2],
        None,
        spatial_total,
        spatial_att_grad,
    )
    spatial_pack_grad = jnp.stack(spatial_parts, axis=2).astype(jnp.bfloat16).reshape(-1, 3 * D)
    spatial_input_grad = weight_grad(spatial_in, spatial_pack_grad, "clip")
    spatial_query_bias = column_sum(spatial_pack_grad[:, 0:D])
    spatial_value_bias = column_sum(spatial_pack_grad[:, 2 * D : 3 * D])
    spatial_in_grad = input_grad(spatial_pack_grad, matrices[0]).reshape(values.shape)
    scale_first_grad = clip_sum(spatial_in_grad * normed_first)
    shift_first_grad = clip_sum(spatial_in_grad)
    patch_gradient = spatial_grad_full + normalize_back(
        normed_first, inverse_first, spatial_in_grad * (1.0 + scale_first)
    )
    modulation_grad = jnp.stack(
        [
            shift_first_grad,
            scale_first_grad,
            gate_first_grad,
            shift_second_grad,
            scale_second_grad,
            gate_second_grad,
        ],
        axis=1,
    ).reshape(clip_local, 6 * D)
    timestep_gradient = frame_total(modulation_grad.reshape(-1, D)).reshape(clip_local, 6 * D)
    table_term = jnp.sum(modulation_grad, axis=0)
    bias_term = jnp.concatenate(
        [
            spatial_query_bias,
            spatial_value_bias,
            spatial_output_bias,
            temporal_query_bias,
            temporal_value_bias,
            temporal_output_bias,
            cross_query_bias,
            pair_value_bias,
            cross_output_bias,
            expand_bias,
            contract_bias,
        ]
    )
    bias_gradient, table_gradient = reduce_vectors(bias_term, table_term)
    final = (
        spatial_input_grad,
        spatial_output_grad,
        temporal_input_grad,
        temporal_output_grad,
        cross_query_grad,
        reduce_columns(pair_weight_grad),
        cross_output_grad,
        expand_grad,
        contract_grad,
    )
    return (
        output,
        patch_gradient,
        caption_gradient,
        timestep_gradient,
        final[0],
        final[1],
        final[2],
        final[3],
        final[4],
        final[5],
        final[6],
        final[7],
        final[8],
        bias_gradient,
        table_gradient,
    )


def solution(mesh):
    placed = (
        P("clip", "frame", None, None),
        P("clip", None, None),
        P("clip"),
        P("clip", None),
        P("frame", "clip"),
        P("frame", "clip"),
        P("frame", "clip"),
        P("frame", "clip"),
        P("frame", "clip"),
        P("frame", "clip"),
        P("frame", "clip"),
        P("frame", "clip"),
        P("frame", "clip"),
        P(("frame", "clip")),
        P(("frame", "clip")),
        P("clip", "frame", None, None),
    )
    return jax.shard_map(
        per_device,
        mesh=mesh,
        in_specs=placed,
        out_specs=(
            P("clip", "frame", None, None),
            P("clip", "frame", None, None),
            P("clip", None, None),
            P("clip", None),
            P("frame", "clip"),
            P("frame", "clip"),
            P("frame", "clip"),
            P("frame", "clip"),
            P("frame", "clip"),
            P("frame", "clip"),
            P("frame", "clip"),
            P("frame", "clip"),
            P("frame", "clip"),
            P(("frame", "clip")),
            P(("frame", "clip")),
        ),
        check_vma=False,
    )
```
